32 devices in a mesh: cls: 8 (over z, y), row: 4 (over x, core).
Axes of the slice: x: 2, y: 2, z: 4, core: 2. Of those that a mesh axis runs over, the one named last changes fastest.
Arguments:
- embeddings: float32 [1024, 1024], P('row'), may hold values from -6 to 6
- weights: float32 [1024, 81920], P(('cls', 'row')), may hold values from -4 to 4
- labels: int32 [1024], replicated, may hold values from 0 to 81919, as said below
Outputs:
- weight_update: float32 [1024, 81920], P(None, ('cls', 'row'))
- losses: float32 [2, 1024], replicated
The draws below stay inside these ranges and needn't reach their ends.
Inputs may be any that keep to these rules, and one draw needn't show every extreme that they name: labels take at most 512 distinct values, at most one in each aligned run of 160 classes; rows may share a label.
All inputs are finite; a program needn't handle non-finite values.
Results may differ from the reference program's by a relative error of at most 0.012.
The reference program's roundings to bfloat16 on the way count: a program that leaves them out, or rounds other values in their place, can miss the bound.
Values may be sent and summed in bfloat16 or wider, within the bound.
No kernel may reach another device: no remote copies, remote signals or barrier semaphores. Data moves between devices by JAX's collectives and lax.ppermute only.
A program may use at most 128 MiB of HBM per device.

```python
import math
import jax
import jax.numpy as jnp
from jax import lax

D = 1024
CLS_DEV = 2560
STEPS = 2
ROWS = 1024
CLASSES = 81920


def embedding_draw(key):
    noise = jax.random.normal(jax.random.fold_in(key, 7), (ROWS, D), jnp.float32)
    return jnp.clip(noise + 0.5, -6.0, 6.0)


def draw_embeddings(key, part):
    return embedding_draw(key)


def draw_weights(key, part):
    base = jax.random.normal(jax.random.fold_in(key, 9), (D, CLASSES), jnp.float32) * (8.0 / math.sqrt(D))
    base = jnp.clip(base, -4.0, 4.0)
    return base


def draw_labels(key, part):
    run_width = CLASSES // 512
    slots = jax.random.randint(jax.random.fold_in(key, 21), (ROWS,), 0, 512, dtype=jnp.int32)
    slots = slots.at[0].set(0).at[ROWS - 1].set(511)
    offsets = jax.random.randint(jax.random.fold_in(key, 22), (512,), 0, run_width, dtype=jnp.int32)
    offsets = offsets.at[0].set(0).at[511].set(run_width - 1)
    return (slots * run_width + offsets[slots]).astype(jnp.int32)


def setup_inputs(seed: int = 0) -> dict:
    arg_keys = jax.random.split(jax.random.key(seed), 4)
    return {
        "embeddings": draw_embeddings(jax.random.fold_in(arg_keys[3], 71), 0),
        "weights": draw_weights(jax.random.fold_in(arg_keys[3], 71), 0),
        "labels": draw_labels(jax.random.fold_in(arg_keys[3], 71), 0),
    }


learn_rate = 2.0


def reference(embeddings, weights, labels):
    rounded = embeddings.astype(jnp.bfloat16)
    row_count = rounded.shape[0]
    block_count = CLASSES // CLS_DEV
    columns = jnp.arange(CLS_DEV, dtype=jnp.int32)
    starts = jnp.arange(block_count, dtype=jnp.int32) * CLS_DEV
    current = weights
    loss_rows = []
    for step_index in range(STEPS):
        stacked = current.reshape(D, block_count, CLS_DEV).transpose(1, 0, 2)

        def block_stats(operands):
            class_block, start = operands
            logits = jnp.dot(rounded, class_block.astype(jnp.bfloat16), preferred_element_type=jnp.float32)
            block_peak = jnp.max(logits, axis=1)
            block_total = jnp.sum(jnp.exp(logits - block_peak[:, None]), axis=1)
            label_hit = (columns[None, :] + start) == labels[:, None]
            block_picked = jnp.sum(jnp.where(label_hit, logits, jnp.float32(0.0)), axis=1)
            return block_peak, block_total, block_picked

        peaks, totals, pickeds = lax.map(block_stats, (stacked, starts))
        row_peak = jnp.max(peaks, axis=0)
        row_total = jnp.sum(totals * jnp.exp(peaks - row_peak[None, :]), axis=0)
        picked = jnp.sum(pickeds, axis=0)
        log_norm = row_peak + jnp.log(row_total)
        loss_rows.append(log_norm - picked)

        def block_update(operands):
            class_block, start = operands
            logits = jnp.dot(rounded, class_block.astype(jnp.bfloat16), preferred_element_type=jnp.float32)
            label_hit = (columns[None, :] + start) == labels[:, None]
            onehot = jnp.where(label_hit, jnp.float32(1.0), jnp.float32(0.0))
            residual = (jnp.exp(logits - log_norm[:, None]) - onehot).astype(jnp.bfloat16)
            gradient = jnp.dot(rounded.T, residual, preferred_element_type=jnp.float32) / row_count
            return class_block - learn_rate * gradient

        renewed = lax.map(block_update, (stacked, starts))
        current = renewed.transpose(1, 0, 2).reshape(D, CLASSES)
    return current - weights, jnp.stack(loss_rows)
```

```python
import jax
import jax.numpy as jnp
from jax import lax
from jax.sharding import PartitionSpec as P

STEPS = 2
AXES = ("cls", "row")

learn_rate = 2.0


def gather_rows(block):
    group = lax.axis_size("row")
    mine = lax.axis_index("row")
    height = block.shape[0]
    whole = jnp.zeros((height * group, block.shape[1]), block.dtype)
    whole = lax.dynamic_update_slice(whole, block, (mine * height, 0))
    paired = group & (group - 1) == 0
    for k in range(1, group):
        if paired:
            source = mine ^ k
            hops = [(i, i ^ k) for i in range(group)]
        else:
            source = (mine - k) % group
            hops = [(i, (i + k) % group) for i in range(group)]
        whole = lax.dynamic_update_slice(
            whole, lax.ppermute(block, "row", hops), (source * height, 0)
        )
    return whole


def exchange(logits, label_hit):
    peers = lax.axis_size(AXES)
    peak = jnp.max(logits, axis=1)
    mass = peak + jnp.log(jnp.sum(jnp.exp(logits - peak[:, None]), axis=1))
    picked = jnp.sum(jnp.where(label_hit, logits, 0.0), axis=1)
    packed = jnp.concatenate([mass.reshape(-1, 128), picked.reshape(-1, 128)])
    sent = jnp.broadcast_to(packed[None], (peers, *packed.shape))
    got = lax.all_to_all(sent, AXES, 0, 0, tiled=True)
    half = packed.shape[0] // 2
    masses = got[:, :half]
    top = jnp.max(masses, axis=0)
    log_norm = top + jnp.log(jnp.sum(jnp.exp(masses - top), axis=0))
    picked = jnp.sum(got[:, half:], axis=0)
    return log_norm.reshape(-1), picked.reshape(-1)


def shards(embeddings, weights, labels):
    peers = lax.axis_size(AXES)
    feature_rows = weights.shape[0]
    class_count = weights.shape[1] // peers
    examples = gather_rows(embeddings.astype(jnp.bfloat16))
    row_count = examples.shape[0]
    rate = learn_rate / row_count
    pieces = weights.astype(jnp.bfloat16).reshape(feature_rows, peers, class_count)
    block = lax.all_to_all(pieces.transpose(1, 0, 2), AXES, 0, 0, tiled=True)
    block = block.reshape(feature_rows * peers, class_count)
    gram = lax.dot_general(
        examples, examples, (((1,), (1,)), ((), ())), preferred_element_type=jnp.float32
    )
    gram = (gram * rate).astype(jnp.bfloat16)
    offset = lax.axis_index(AXES) * class_count
    columns = lax.broadcasted_iota(jnp.int32, (1, class_count), 1) + offset
    label_hit = columns == labels[:, None]
    onehot = jnp.where(label_hit, 1.0, 0.0)
    logits = jnp.dot(examples, block, preferred_element_type=jnp.float32)
    loss_rows = []
    total = 0.0
    for step_index in range(STEPS):
        if step_index > 0:
            logits = logits - jnp.dot(gram, residual, preferred_element_type=jnp.float32)
        log_norm, picked = exchange(logits, label_hit)
        loss_rows.append(log_norm - picked)
        residual = jnp.exp(logits - log_norm[:, None]) - onehot
        total = total + residual
        residual = residual.astype(jnp.bfloat16)
    update = lax.dot_general(
        examples,
        total.astype(jnp.bfloat16),
        (((0,), (0,)), ((), ())),
        preferred_element_type=jnp.float32,
    )
    return (update * -rate, jnp.stack(loss_rows))


def solution(mesh):
    placed = (P("row", None), P(AXES, None), P())
    return jax.shard_map(
        shards,
        mesh=mesh,
        in_specs=placed,
        out_specs=(P(None, AXES), P()),
        check_vma=False,
    )
```

```python
import functools

import jax
import jax.numpy as jnp
from jax import lax
from jax.experimental import pallas as pl
from jax.experimental.pallas import tpu as pltpu
from jax.sharding import PartitionSpec as P

AXES = ("cls", "row")
LANES = 128
MIB = 1 << 20

learn_rate = 2.0

WHOLE = pl.BlockSpec(memory_space=pltpu.VMEM)


def tile(width):
    return next(t for t in (512, 256, 128) if width % t == 0)


def diagonal():
    rows = lax.broadcasted_iota(jnp.int32, (LANES, LANES), 0)
    lanes = lax.broadcasted_iota(jnp.int32, (LANES, LANES), 1)
    return rows == lanes


def to_row(column):
    keep = diagonal()
    parts = []
    for start in range(0, column.shape[0], LANES):
        spread = jnp.broadcast_to(column[start : start + LANES], (LANES, LANES))
        parts.append(jnp.sum(jnp.where(keep, spread, 0.0), axis=0, keepdims=True))
    return jnp.concatenate(parts, axis=1)


def to_column(row):
    keep = diagonal()
    parts = []
    for start in range(0, row.shape[1], LANES):
        spread = jnp.broadcast_to(row[:, start : start + LANES], (LANES, LANES))
        parts.append(jnp.sum(jnp.where(keep, spread, 0.0), axis=1, keepdims=True))
    return jnp.concatenate(parts, axis=0)


def combine(got):
    masses = got[:, 0:1, :]
    top = jnp.max(masses, axis=0)
    log_norm = top + jnp.log(jnp.sum(jnp.exp(masses - top[None]), axis=0))
    return log_norm, jnp.sum(got[:, 1:2, :], axis=0)


def tally(logits, hits, first, peak_ref, mass_ref, pick_ref):
    groups = [logits[:, g : g + LANES] for g in range(0, logits.shape[1], LANES)]
    peak = functools.reduce(jnp.maximum, groups)
    if not first:
        peak = jnp.maximum(peak, peak_ref[...])
    mass = sum(jnp.exp(g - peak) for g in groups)
    pick = sum(jnp.where(h, g, 0.0) for g, h in zip(groups, hits))
    if not first:
        mass = mass + mass_ref[...] * jnp.exp(peak_ref[...] - peak)
        pick = pick + pick_ref[...]
    peak_ref[...] = peak
    mass_ref[...] = mass
    pick_ref[...] = pick


def finish(out_ref, peak_ref, mass_ref, pick_ref):
    lanes_peak = peak_ref[...]
    peak = jnp.max(lanes_peak, axis=1, keepdims=True)
    mass = jnp.sum(mass_ref[...] * jnp.exp(lanes_peak - peak), axis=1, keepdims=True)
    pick = jnp.sum(pick_ref[...], axis=1, keepdims=True)
    rows = jnp.concatenate([to_row(peak + jnp.log(mass)), to_row(pick)], axis=0)
    out_ref[...] = jnp.broadcast_to(rows[None], out_ref.shape)


def hits_of(places, start, width):
    lane = lax.broadcasted_iota(jnp.int32, (1, LANES), 1)
    return [places == lane + (start + g) for g in range(0, width, LANES)]


def cast_kernel(in_ref, out_ref):
    width = out_ref.shape[2]
    for k in range(out_ref.shape[0]):
        out_ref[k] = in_ref[:, k * width : (k + 1) * width].astype(out_ref.dtype)


def first_kernel(places_ref, x_ref, w_ref, logits_ref, sent_ref, peak_ref, mass_ref, pick_ref):
    width = w_ref.shape[1]
    step = tile(width)
    places = places_ref[...]
    for start in range(0, width, step):
        block = slice(start, start + step)
        logits = jnp.dot(x_ref[...], w_ref[:, block], preferred_element_type=jnp.float32)
        logits_ref[:, block] = logits
        tally(logits, hits_of(places, start, step), start == 0, peak_ref, mass_ref, pick_ref)
    finish(sent_ref, peak_ref, mass_ref, pick_ref)


def second_kernel(
    got_ref, places_ref, gram_ref, old_ref,
    residual_ref, logits_ref, sent_ref, peak_ref, mass_ref, pick_ref,
):
    width = old_ref.shape[1]
    step = tile(width)
    log_norm, _ = combine(got_ref[...])
    norm = to_column(log_norm)
    places = places_ref[...]
    for start in range(0, width, step):
        block = slice(start, start + step)
        hits = hits_of(places, start, step)
        old = old_ref[:, block]
        chance = jnp.exp(old - norm)
        onehot = jnp.concatenate([jnp.where(h, 1.0, 0.0) for h in hits], axis=1)
        residual = (chance - onehot).astype(jnp.bfloat16)
        residual_ref[:, block] = residual
        logits = old - jnp.dot(gram_ref[...], residual, preferred_element_type=jnp.float32)
        logits_ref[:, block] = logits
        tally(logits, hits, start == 0, peak_ref, mass_ref, pick_ref)
    finish(sent_ref, peak_ref, mass_ref, pick_ref)


def last_kernel(
    rate, before_ref, got_ref, places_ref, flipped_ref, residual_ref, logits_ref,
    update_ref, losses_ref, buffer_ref, sems,
):
    width = logits_ref.shape[1]
    step = tile(width)
    old_norm, old_pick = combine(before_ref[...])
    log_norm, pick = combine(got_ref[...])
    losses_ref[...] = jnp.concatenate([old_norm - old_pick, log_norm - pick], axis=0)
    norm = to_column(log_norm)
    places = places_ref[...]

    def copy(start):
        slot = start // step % 2
        return pltpu.make_async_copy(
            buffer_ref.at[slot], update_ref.at[:, pl.ds(start, step)], sems.at[slot]
        )

    for start in range(0, width, step):
        block = slice(start, start + step)
        hits = hits_of(places, start, step)
        chance = jnp.exp(logits_ref[:, block] - norm)
        onehot = jnp.concatenate([jnp.where(h, 1.0, 0.0) for h in hits], axis=1)
        total = residual_ref[:, block].astype(jnp.float32) + (chance - onehot)
        update = jnp.dot(
            flipped_ref[...], total.astype(jnp.bfloat16), preferred_element_type=jnp.float32
        )
        if start >= 2 * step:
            copy(start - 2 * step).wait()
        buffer_ref[start // step % 2] = update * -rate
        copy(start).start()
    for start in range(max(0, width - 2 * step), width, step):
        copy(start).wait()


def grant(mib):
    return pltpu.CompilerParams(vmem_limit_bytes=mib * MIB)


def gather_rows(block):
    group = lax.axis_size("row")
    mine = lax.axis_index("row")
    height = block.shape[0]
    whole = jnp.zeros((height * group, block.shape[1]), block.dtype)
    whole = lax.dynamic_update_slice(whole, block, (mine * height, 0))
    paired = group & (group - 1) == 0
    for k in range(1, group):
        if paired:
            source = mine ^ k
            hops = [(i, i ^ k) for i in range(group)]
        else:
            source = (mine - k) % group
            hops = [(i, (i + k) % group) for i in range(group)]
        whole = lax.dynamic_update_slice(
            whole, lax.ppermute(block, "row", hops), (source * height, 0)
        )
    return whole


def trade(sent):
    return lax.all_to_all(sent, AXES, 0, 0, tiled=True)


def shards(embeddings, weights, labels):
    peers = lax.axis_size(AXES)
    depth = weights.shape[0]
    classes = weights.shape[1] // peers
    f32, bf16 = jnp.float32, jnp.bfloat16
    chunk = 4 if peers % 4 == 0 else 1
    pieces = pl.pallas_call(
        cast_kernel,
        grid=(peers // chunk,),
        in_specs=[pl.BlockSpec((depth, chunk * classes), lambda i: (0, i))],
        out_specs=pl.BlockSpec((chunk, depth, classes), lambda i: (i, 0, 0)),
        out_shape=jax.ShapeDtypeStruct((peers, depth, classes), bf16),
    )(weights)
    block = lax.all_to_all(pieces, AXES, 0, 0, tiled=True)
    block = block.reshape(depth * peers, classes)

    examples = gather_rows(embeddings.astype(bf16))
    rows = examples.shape[0]
    rate = learn_rate / rows
    gram = lax.dot_general(examples, examples, (((1,), (1,)), ((), ())), preferred_element_type=f32)
    gram = (gram * rate).astype(bf16)
    flipped = examples.T
    places = labels - lax.axis_index(AXES) * classes
    places = jnp.broadcast_to(places[:, None], (rows, LANES))

    logits_shape = pltpu.VMEM((rows, classes), f32)
    stats_shape = jax.ShapeDtypeStruct((peers, 2, rows), f32)
    scratch = [pltpu.VMEM((rows, LANES), f32)] * 3
    logits, sent = pl.pallas_call(
        first_kernel,
        in_specs=[WHOLE] * 3,
        out_specs=[WHOLE] * 2,
        out_shape=[logits_shape, stats_shape],
        scratch_shapes=scratch,
        compiler_params=grant(16),
    )(places, examples, block)
    before = trade(sent)
    residual, logits, sent = pl.pallas_call(
        second_kernel,
        in_specs=[WHOLE] * 4,
        out_specs=[WHOLE] * 3,
        out_shape=[pltpu.VMEM((rows, classes), bf16), logits_shape, stats_shape],
        scratch_shapes=scratch,
        compiler_params=grant(16),
    )(before, places, gram, logits)
    got = trade(sent)
    step = tile(classes)
    update, losses = pl.pallas_call(
        functools.partial(last_kernel, rate),
        in_specs=[WHOLE] * 6,
        out_specs=[pl.BlockSpec(memory_space=pltpu.HBM), WHOLE],
        out_shape=[
            jax.ShapeDtypeStruct((depth * peers, classes), f32),
            jax.ShapeDtypeStruct((2, rows), f32),
        ],
        scratch_shapes=[pltpu.VMEM((2, depth * peers, step), f32), pltpu.SemaphoreType.DMA((2,))],
        compiler_params=grant(16),
    )(before, got, places, flipped, residual, logits)
    return update, losses


def solution(mesh):
    placed = (P("row", None), P(AXES, None), P())
    return jax.shard_map(
        shards,
        mesh=mesh,
        in_specs=placed,
        out_specs=(P(None, AXES), P()),
        check_vma=False,
    )
```

```python
import functools

import jax
import jax.numpy as jnp
from jax import lax
from jax.experimental import pallas as pl
from jax.experimental.pallas import tpu as pltpu
from jax.sharding import PartitionSpec as P

AXES = ("cls", "row")
LANES = 128
LOG2E = 1.4426950408889634
MIB = 1 << 20

learn_rate = 2.0

WHOLE = pl.BlockSpec(memory_space=pltpu.VMEM)
ANYWHERE = pl.BlockSpec(memory_space=pltpu.HBM)


def blocks_of(width):
    step = next(t for t in (512, 256, 128) if width % t == 0)
    widths = [step] * (width // step)
    starts = [sum(widths[:k]) for k in range(len(widths))]
    return [slice(start, start + size) for start, size in zip(starts, widths)]


def diagonal():
    rows = lax.broadcasted_iota(jnp.int32, (LANES, LANES), 0)
    lanes = lax.broadcasted_iota(jnp.int32, (LANES, LANES), 1)
    return rows == lanes


def to_row(column):
    keep = diagonal()
    parts = []
    for start in range(0, column.shape[0], LANES):
        spread = jnp.broadcast_to(column[start : start + LANES], (LANES, LANES))
        parts.append(jnp.sum(jnp.where(keep, spread, 0.0), axis=0, keepdims=True))
    return jnp.concatenate(parts, axis=1)


def to_column(row):
    keep = diagonal()
    parts = []
    for start in range(0, row.shape[1], LANES):
        spread = jnp.broadcast_to(row[:, start : start + LANES], (LANES, LANES))
        parts.append(jnp.sum(jnp.where(keep, spread, 0.0), axis=1, keepdims=True))
    return jnp.concatenate(parts, axis=0)


def combine(masses):
    top = jnp.max(masses, axis=0)
    return top + jnp.log(jnp.sum(jnp.exp2(masses - top[None]), axis=0)) * LOG2E


def tally(logits, hits, first, peak_ref, mass_ref, pick_ref):
    groups = [logits[:, g : g + LANES] for g in range(0, logits.shape[1], LANES)]
    peak = functools.reduce(jnp.maximum, groups)
    if not first:
        peak = jnp.maximum(peak, peak_ref[...])
    mass = functools.reduce(jnp.add, [jnp.exp2(g - peak) for g in groups])
    pick = functools.reduce(jnp.add, [jnp.where(h, g, 0.0) for g, h in zip(groups, hits)])
    if not first:
        mass = mass + mass_ref[...] * jnp.exp2(peak_ref[...] - peak)
        pick = pick + pick_ref[...]
    peak_ref[...] = peak
    mass_ref[...] = mass
    pick_ref[...] = pick


def finish(peak_ref, mass_ref, pick_ref):
    lanes_peak = peak_ref[...]
    peak = jnp.max(lanes_peak, axis=1, keepdims=True)
    mass = jnp.sum(mass_ref[...] * jnp.exp2(lanes_peak - peak), axis=1, keepdims=True)
    pick = jnp.sum(pick_ref[...], axis=1, keepdims=True)
    return to_row(peak + jnp.log(mass) * LOG2E), to_row(pick)


def spread(row, peers):
    return jnp.broadcast_to(row[None], (peers, *row.shape))


def hits_of(places, block):
    lane = lax.broadcasted_iota(jnp.int32, (1, LANES), 1)
    return [places == lane + g for g in range(block.start, block.stop, LANES)]


def onehot(hits):
    return jnp.concatenate([jnp.where(h, 1.0, 0.0) for h in hits], axis=1)


def cast_kernel(in_ref, out_ref):
    width = out_ref.shape[2]
    for k in range(out_ref.shape[0]):
        out_ref[k] = in_ref[:, k * width : (k + 1) * width].astype(out_ref.dtype)


def first_kernel(places_ref, x_ref, w_ref, logits_ref, sent_ref, peak_ref, mass_ref, pick_ref):
    stats = (peak_ref, mass_ref, pick_ref)
    places = places_ref[...]
    depth = x_ref.shape[1]
    for k, block in enumerate(blocks_of(w_ref.shape[2])):
        taken = w_ref[:, :, block].reshape(depth, block.stop - block.start)
        logits = jnp.dot(x_ref[...], taken, preferred_element_type=jnp.float32) * LOG2E
        logits_ref[:, block] = logits
        tally(logits, hits_of(places, block), k == 0, *stats)
    mass, pick = finish(*stats)
    peers, rows = sent_ref.shape[0], x_ref.shape[0]
    share = peers * LANES // rows
    sent_ref[:, :, :rows] = spread(mass, peers)
    for g in range(rows // LANES):
        sent_ref[g * share : (g + 1) * share, :, rows:] = spread(
            pick[:, g * LANES : (g + 1) * LANES], share
        )


def second_kernel(
    got_ref, places_ref, gram_ref, old_ref,
    residual_ref, logits_ref, norm_ref, sent_ref, peak_ref, mass_ref, pick_ref,
):
    rows = old_ref.shape[0]
    stats = (peak_ref, mass_ref, pick_ref)
    log_norm = combine(got_ref[:, :, :rows])
    norm_ref[...] = log_norm
    norm = to_column(log_norm)
    places = places_ref[...]
    blocks = blocks_of(old_ref.shape[1])

    for k, block in enumerate(blocks):
        hits = hits_of(places, block)
        old = old_ref[:, block]
        residual = (jnp.exp2(old - norm) - onehot(hits)).astype(jnp.bfloat16)
        residual_ref[:, block] = residual
        logits = old - jnp.dot(gram_ref[...], residual, preferred_element_type=jnp.float32)
        logits_ref[:, block] = logits
        tally(logits, hits, k == 0, *stats)
    mass, pick = finish(*stats)
    peers = sent_ref.shape[0]
    sent_ref[:, :, :rows] = spread(mass, peers)
    sent_ref[:, :, rows : 2 * rows] = spread(pick, peers)
    sent_ref[:, :, 2 * rows :] = spread(jnp.sum(got_ref[:, :, rows:], axis=0), peers)


def last_kernel(
    norm_ref, got_ref, places_ref, flipped_ref, residual_ref, logits_ref,
    update_hbm, losses_ref, update_ref, sems,
):
    rows = logits_ref.shape[0]
    share = got_ref.shape[0] * LANES // rows
    log_norm = combine(got_ref[:, :, :rows])
    pick = jnp.sum(got_ref[:, :, rows : 2 * rows], axis=0)
    old_pick = jnp.concatenate(
        [got_ref[g * share, :, 2 * rows :] for g in range(rows // LANES)], axis=1
    )
    losses = jnp.concatenate([norm_ref[...] - old_pick, log_norm - pick], axis=0)
    losses_ref[...] = losses * (1.0 / LOG2E)
    norm = to_column(log_norm)
    places = places_ref[...]
    blocks = blocks_of(logits_ref.shape[1])
    slots = update_ref.shape[0]

    def copy(k):
        size = blocks[k].stop - blocks[k].start
        return pltpu.make_async_copy(
            update_ref.at[k % slots, :, pl.ds(0, size)],
            update_hbm.at[:, pl.ds(blocks[k].start, size)],
            sems.at[k % slots],
        )

    for k, block in enumerate(blocks):
        chance = jnp.exp2(logits_ref[:, block] - norm)
        total = residual_ref[:, block].astype(jnp.float32)
        total = total + (chance - onehot(hits_of(places, block)))
        update = jnp.dot(
            flipped_ref[...], total.astype(jnp.bfloat16), preferred_element_type=jnp.float32
        )
        if k >= slots:
            copy(k - slots).wait()
        update_ref[k % slots, :, : block.stop - block.start] = update
        copy(k).start()
    for k in range(max(0, len(blocks) - slots), len(blocks)):
        copy(k).wait()


def grant(mib):
    return pltpu.CompilerParams(vmem_limit_bytes=mib * MIB)


def assemble_kernel(rate, sources_ref, *refs):
    *block_refs, x_ref, gram_ref, flipped_ref = refs
    height = block_refs[0].shape[0]
    for k, block_ref in enumerate(block_refs):
        x_ref[pl.ds(pl.multiple_of(sources_ref[k] * height, height), height), :] = block_ref[...]
    examples = x_ref[...]
    gram = lax.dot_general(
        examples, examples, (((1,), (1,)), ((), ())), preferred_element_type=jnp.float32
    )
    gram_ref[...] = (gram * (rate * LOG2E)).astype(gram_ref.dtype)
    flipped_ref[...] = (examples.T * -rate).astype(flipped_ref.dtype)


def neighbours(block):
    group = lax.axis_size("row")
    mine = lax.axis_index("row")
    paired = group & (group - 1) == 0
    sources, blocks = [mine], [block]
    for k in range(1, group):
        if paired:
            sources.append(mine ^ k)
            hops = [(i, i ^ k) for i in range(group)]
        else:
            sources.append((mine - k) % group)
            hops = [(i, (i + k) % group) for i in range(group)]
        blocks.append(lax.ppermute(block, "row", hops))
    return jnp.stack(sources).astype(jnp.int32), blocks


def near(array):
    return pltpu.with_memory_space_constraint(array, pltpu.VMEM)


def away(array):
    return pltpu.with_memory_space_constraint(array, pltpu.HBM)


def trade(sent):
    return lax.all_to_all(sent, AXES, 0, 0, tiled=True)


def shards(embeddings, weights, labels):
    peers = lax.axis_size(AXES)
    depth = weights.shape[0]
    classes = weights.shape[1] // peers
    f32, bf16 = jnp.float32, jnp.bfloat16
    chunk = 4 if peers % 4 == 0 else 1
    pieces = pl.pallas_call(
        cast_kernel,
        grid=(peers // chunk,),
        in_specs=[pl.BlockSpec((depth, chunk * classes), lambda i: (0, i))],
        out_specs=pl.BlockSpec((chunk, depth, classes), lambda i: (i, 0, 0)),
        out_shape=pltpu.HBM((peers, depth, classes), bf16),
    )(away(weights))
    block = lax.all_to_all(pieces, AXES, 0, 0, tiled=True)

    rows = labels.shape[0]
    rate = learn_rate / rows
    places = labels - lax.axis_index(AXES) * classes
    places = jnp.broadcast_to(places[:, None], (rows, LANES))
    sources, blocks = neighbours(embeddings.astype(bf16))
    examples, gram, flipped = pl.pallas_call(
        functools.partial(assemble_kernel, rate),
        in_specs=[pl.BlockSpec(memory_space=pltpu.SMEM)] + [WHOLE] * len(blocks),
        out_specs=[WHOLE] * 3,
        out_shape=[
            pltpu.VMEM((rows, depth * peers), bf16),
            pltpu.HBM((rows, rows), bf16),
            pltpu.HBM((depth * peers, rows), bf16),
        ],
        compiler_params=grant(16),
    )(sources, *blocks)

    logits_shape = pltpu.VMEM((rows, classes), f32)
    scratch = [pltpu.VMEM((rows, LANES), f32)] * 3
    blocks = blocks_of(classes)
    widest, slots = max(b.stop - b.start for b in blocks), min(3, len(blocks))
    logits, sent = pl.pallas_call(
        first_kernel,
        in_specs=[WHOLE] * 3,
        out_specs=[WHOLE] * 2,
        out_shape=[logits_shape, jax.ShapeDtypeStruct((peers, 1, rows + LANES), f32)],
        scratch_shapes=scratch,
        compiler_params=grant(16),
    )(places, near(examples), near(block))
    residual, logits, norm, sent = pl.pallas_call(
        second_kernel,
        in_specs=[WHOLE] * 4,
        out_specs=[WHOLE] * 4,
        out_shape=[
            pltpu.VMEM((rows, classes), bf16),
            logits_shape,
            jax.ShapeDtypeStruct((1, rows), f32),
            jax.ShapeDtypeStruct((peers, 1, 2 * rows + LANES), f32),
        ],
        scratch_shapes=scratch,
        compiler_params=grant(17),
    )(trade(sent), places, gram, near(logits))
    update, losses = pl.pallas_call(
        last_kernel,
        in_specs=[WHOLE] * 6,
        out_specs=[ANYWHERE, WHOLE],
        out_shape=[
            jax.ShapeDtypeStruct((depth * peers, classes), f32),
            jax.ShapeDtypeStruct((2, rows), f32),
        ],
        scratch_shapes=[
            pltpu.VMEM((slots, depth * peers, widest), f32),
            pltpu.SemaphoreType.DMA((slots,)),
        ],
        compiler_params=grant(16),
    )(norm, trade(sent), places, flipped, near(residual), near(logits))
    return update, losses


def solution(mesh):
    placed = (P("row", None), P(AXES, None), P())
    return jax.shard_map(
        shards,
        mesh=mesh,
        in_specs=placed,
        out_specs=(P(None, AXES), P()),
        check_vma=False,
    )
```

```python
import functools

import jax
import jax.numpy as jnp
from jax import lax
from jax.experimental import pallas as pl
from jax.experimental.pallas import tpu as pltpu
from jax.sharding import PartitionSpec as P

AXES = ("cls", "row")
LANES = 128
LOG2E = 1.4426950408889634
MIB = 1 << 20

learn_rate = 2.0

WHOLE = pl.BlockSpec(memory_space=pltpu.VMEM)
ANYWHERE = pl.BlockSpec(memory_space=pltpu.HBM)


def blocks_of(width):
    step = next(t for t in (512, 256, 128) if width % t == 0)
    widths = [step] * (width // step)
    starts = [sum(widths[:k]) for k in range(len(widths))]
    return [slice(start, start + size) for start, size in zip(starts, widths)]


def diagonal():
    rows = lax.broadcasted_iota(jnp.int32, (LANES, LANES), 0)
    lanes = lax.broadcasted_iota(jnp.int32, (LANES, LANES), 1)
    return rows == lanes


def to_row(column):
    keep = diagonal()
    parts = []
    for start in range(0, column.shape[0], LANES):
        spread = jnp.broadcast_to(column[start : start + LANES], (LANES, LANES))
        parts.append(jnp.sum(jnp.where(keep, spread, 0.0), axis=0, keepdims=True))
    return jnp.concatenate(parts, axis=1)


def to_column(row):
    keep = diagonal()
    parts = []
    for start in range(0, row.shape[1], LANES):
        spread = jnp.broadcast_to(row[:, start : start + LANES], (LANES, LANES))
        parts.append(jnp.sum(jnp.where(keep, spread, 0.0), axis=1, keepdims=True))
    return jnp.concatenate(parts, axis=0)


def combine(masses):
    top = jnp.max(masses, axis=0)
    return top + jnp.log(jnp.sum(jnp.exp2(masses - top[None]), axis=0)) * LOG2E


def tally(logits, hits, first, peak_ref, mass_ref, pick_ref):
    groups = [logits[:, g : g + LANES] for g in range(0, logits.shape[1], LANES)]
    peak = functools.reduce(jnp.maximum, groups)
    if not first:
        peak = jnp.maximum(peak, peak_ref[...])
    mass = functools.reduce(jnp.add, [jnp.exp2(g - peak) for g in groups])
    pick = jnp.zeros_like(peak) if first else pick_ref[...]
    for g, h in zip(groups, hits):
        pick = jnp.where(h, g, pick)
    if not first:
        mass = mass + mass_ref[...] * jnp.exp2(peak_ref[...] - peak)
    peak_ref[...] = peak
    mass_ref[...] = mass
    pick_ref[...] = pick


def finish(peak_ref, mass_ref, pick_ref):
    lanes_peak = peak_ref[...]
    peak = jnp.max(lanes_peak, axis=1, keepdims=True)
    mass = jnp.sum(mass_ref[...] * jnp.exp2(lanes_peak - peak), axis=1, keepdims=True)
    pick = jnp.sum(pick_ref[...], axis=1, keepdims=True)
    return to_row(peak + jnp.log(mass) * LOG2E), to_row(pick)


def spread(row, peers):
    return jnp.broadcast_to(row[None], (peers, *row.shape))


def hits_of(places, block):
    lane = lax.broadcasted_iota(jnp.int32, (1, LANES), 1).astype(places.dtype)
    return [places == lane + g for g in range(block.start, block.stop, LANES)]


def onehot(hits):
    return jnp.concatenate([jnp.where(h, 1.0, 0.0) for h in hits], axis=1)


def cast_kernel(in_hbm, out_hbm, wide_ref, slim_ref, in_sems, out_sems):
    ahead, chunk, _, width = slim_ref.shape
    steps = out_hbm.shape[0] // chunk

    def load(n):
        span = pl.ds(n * chunk * width, chunk * width)
        slot = n % ahead
        return pltpu.make_async_copy(in_hbm.at[:, span], wide_ref.at[slot], in_sems.at[slot])

    def store(n):
        slot = n % ahead
        return pltpu.make_async_copy(
            slim_ref.at[slot], out_hbm.at[pl.ds(n * chunk, chunk)], out_sems.at[slot]
        )

    for n in range(min(ahead, steps)):
        load(n).start()
    for n in range(steps):
        load(n).wait()
        if n >= ahead:
            store(n - ahead).wait()
        for k in range(chunk):
            piece = wide_ref[n % ahead, :, k * width : (k + 1) * width]
            slim_ref[n % ahead, k] = piece.astype(slim_ref.dtype)
        store(n).start()
        if n + ahead < steps:
            load(n + ahead).start()
    for n in range(max(0, steps - ahead), steps):
        store(n).wait()


def first_kernel(
    places_ref, x_hbm, w_hbm, logits_ref, sent_ref, x_ref, w_ref, peak_ref, mass_ref, pick_ref, sems
):
    stats = (peak_ref, mass_ref, pick_ref)
    depth = x_ref.shape[1]
    blocks = blocks_of(w_ref.shape[2])
    spans = [slice(0, blocks[0].stop), slice(blocks[0].stop, w_ref.shape[2])]
    copies = [pltpu.make_async_copy(x_hbm, x_ref, sems.at[2])]
    for n, span in enumerate(spans[: len(blocks)]):
        part = pl.ds(span.start, span.stop - span.start)
        copies.append(
            pltpu.make_async_copy(w_hbm.at[:, :, part], w_ref.at[:, :, part], sems.at[n])
        )
    for copy in copies:
        copy.start()
    places = places_ref[...]
    copies[0].wait()
    for k, block in enumerate(blocks):
        if k < 2:
            copies[k + 1].wait()
        taken = w_ref[:, :, block].reshape(depth, block.stop - block.start)
        logits = jnp.dot(x_ref[...], taken, preferred_element_type=jnp.float32) * LOG2E
        logits_ref[:, block] = logits
        tally(logits, hits_of(places, block), k == 0, *stats)
    mass, pick = finish(*stats)
    peers, rows = sent_ref.shape[0], x_ref.shape[0]
    share = peers * LANES // rows
    sent_ref[:, :, :rows] = spread(mass, peers)
    for g in range(rows // LANES):
        sent_ref[g * share : (g + 1) * share, :, rows:] = spread(
            pick[:, g * LANES : (g + 1) * LANES], share
        )


def second_kernel(
    got_ref, places_ref, gram_ref, old_ref,
    residual_ref, logits_ref, norm_ref, sent_ref, peak_ref, mass_ref, pick_ref,
):
    rows = old_ref.shape[0]
    stats = (peak_ref, mass_ref, pick_ref)
    log_norm = combine(got_ref[:, :, :rows])
    norm_ref[...] = log_norm
    norm = to_column(log_norm)
    places = places_ref[...]
    blocks = blocks_of(old_ref.shape[1])

    for k, block in enumerate(blocks):
        hits = hits_of(places, block)
        old = old_ref[:, block]
        residual = (jnp.exp2(old - norm) - onehot(hits)).astype(jnp.bfloat16)
        residual_ref[:, block] = residual
        logits = old - jnp.dot(
            gram_ref[...], residual_ref[:, block], preferred_element_type=jnp.float32
        )
        logits_ref[:, block] = logits
        tally(logits, hits_of(places.astype(jnp.float32), block), k == 0, *stats)
    mass, pick = finish(*stats)
    peers = sent_ref.shape[0]
    sent_ref[:, :, :rows] = spread(mass, peers)
    sent_ref[:, :, rows : 2 * rows] = spread(pick, peers)
    sent_ref[:, :, 2 * rows :] = spread(jnp.sum(got_ref[:, :, rows:], axis=0), peers)


def last_kernel(
    norm_ref, got_ref, places_ref, flipped_ref, residual_ref, logits_ref,
    update_hbm, losses_ref, update_ref, sems,
):
    rows = logits_ref.shape[0]
    share = got_ref.shape[0] * LANES // rows
    log_norm = combine(got_ref[:, :, :rows])
    pick = jnp.sum(got_ref[:, :, rows : 2 * rows], axis=0)
    old_pick = jnp.concatenate(
        [got_ref[g * share, :, 2 * rows :] for g in range(rows // LANES)], axis=1
    )
    losses = jnp.concatenate([norm_ref[...] - old_pick, log_norm - pick], axis=0)
    losses_ref[...] = losses * (1.0 / LOG2E)
    norm = to_column(log_norm)
    places = places_ref[...]
    blocks = blocks_of(logits_ref.shape[1])
    slots = update_ref.shape[0]

    def copy(k):
        size = blocks[k].stop - blocks[k].start
        return pltpu.make_async_copy(
            update_ref.at[k % slots, :, pl.ds(0, size)],
            update_hbm.at[:, pl.ds(blocks[k].start, size)],
            sems.at[k % slots],
        )

    for k, block in enumerate(blocks):
        chance = jnp.exp2(logits_ref[:, block] - norm)
        total = residual_ref[:, block].astype(jnp.float32)
        total = total + (chance - onehot(hits_of(places, block)))
        update = jnp.dot(
            flipped_ref[...], total.astype(jnp.bfloat16), preferred_element_type=jnp.float32
        )
        if k >= slots:
            copy(k - slots).wait()
        update_ref[k % slots, :, : block.stop - block.start] = update
        copy(k).start()
    for k in range(max(0, len(blocks) - slots), len(blocks)):
        copy(k).wait()


def grant(mib):
    return pltpu.CompilerParams(vmem_limit_bytes=mib * MIB)


def assemble_kernel(rate, sources_ref, *refs):
    *block_refs, x_ref, gram_ref, flipped_ref = refs
    height = block_refs[0].shape[0]
    for k, block_ref in enumerate(block_refs):
        x_ref[pl.ds(pl.multiple_of(sources_ref[k] * height, height), height), :] = block_ref[...]
    examples = x_ref[...]
    gram = lax.dot_general(
        examples, examples, (((1,), (1,)), ((), ())), preferred_element_type=jnp.float32
    )
    gram_ref[...] = (gram * (rate * LOG2E)).astype(gram_ref.dtype)
    flipped_ref[...] = (examples.T * -rate).astype(flipped_ref.dtype)


def neighbours(block):
    group = lax.axis_size("row")
    mine = lax.axis_index("row")
    paired = group & (group - 1) == 0
    sources, blocks = [mine], [block]
    for k in range(1, group):
        if paired:
            sources.append(mine ^ k)
            hops = [(i, i ^ k) for i in range(group)]
        else:
            sources.append((mine - k) % group)
            hops = [(i, (i + k) % group) for i in range(group)]
        blocks.append(lax.ppermute(block, "row", hops))
    return jnp.stack(sources).astype(jnp.int32), blocks


def near(array):
    return pltpu.with_memory_space_constraint(array, pltpu.VMEM)


def away(array):
    return pltpu.with_memory_space_constraint(array, pltpu.HBM)


def trade(sent):
    return lax.all_to_all(sent, AXES, 0, 0, tiled=True)


def shards(embeddings, weights, labels):
    peers = lax.axis_size(AXES)
    depth = weights.shape[0]
    classes = weights.shape[1] // peers
    f32, bf16 = jnp.float32, jnp.bfloat16
    chunk = 4 if peers % 4 == 0 else 1
    ahead = min(4, peers // chunk)
    pieces = pl.pallas_call(
        cast_kernel,
        in_specs=[ANYWHERE],
        out_specs=ANYWHERE,
        out_shape=pltpu.HBM((peers, depth, classes), bf16),
        scratch_shapes=[
            pltpu.VMEM((ahead, depth, chunk * classes), f32),
            pltpu.VMEM((ahead, chunk, depth, classes), bf16),
            pltpu.SemaphoreType.DMA((ahead,)),
            pltpu.SemaphoreType.DMA((ahead,)),
        ],
        compiler_params=grant(16),
    )(away(weights))
    block = lax.all_to_all(pieces, AXES, 0, 0, tiled=True)

    rows = labels.shape[0]
    rate = learn_rate / rows
    places = labels - lax.axis_index(AXES) * classes
    places = jnp.broadcast_to(places[:, None], (rows, LANES))
    sources, blocks = neighbours(embeddings.astype(bf16))
    examples, gram, flipped = pl.pallas_call(
        functools.partial(assemble_kernel, rate),
        in_specs=[pl.BlockSpec(memory_space=pltpu.SMEM)] + [WHOLE] * len(blocks),
        out_specs=[WHOLE] * 3,
        out_shape=[
            pltpu.HBM((rows, depth * peers), bf16),
            pltpu.HBM((rows, rows), bf16),
            pltpu.HBM((depth * peers, rows), bf16),
        ],
        compiler_params=grant(16),
    )(sources, *blocks)

    logits_shape = pltpu.VMEM((rows, classes), f32)
    scratch = [pltpu.VMEM((rows, LANES), f32)] * 3
    blocks = blocks_of(classes)
    widest, slots = max(b.stop - b.start for b in blocks), min(3, len(blocks))
    logits, sent = pl.pallas_call(
        first_kernel,
        in_specs=[WHOLE, ANYWHERE, ANYWHERE],
        out_specs=[WHOLE] * 2,
        out_shape=[logits_shape, jax.ShapeDtypeStruct((peers, 1, rows + LANES), f32)],
        scratch_shapes=[
            pltpu.VMEM(examples.shape, bf16),
            pltpu.VMEM(block.shape, bf16),
            *scratch,
            pltpu.SemaphoreType.DMA((3,)),
        ],
        compiler_params=grant(16),
    )(places, away(examples), away(block))
    residual, logits, norm, sent = pl.pallas_call(
        second_kernel,
        in_specs=[WHOLE] * 4,
        out_specs=[WHOLE] * 4,
        out_shape=[
            pltpu.VMEM((rows, classes), bf16),
            logits_shape,
            jax.ShapeDtypeStruct((1, rows), f32),
            jax.ShapeDtypeStruct((peers, 1, 2 * rows + LANES), f32),
        ],
        scratch_shapes=scratch,
        compiler_params=grant(17),
    )(trade(sent), places, gram, near(logits))
    update, losses = pl.pallas_call(
        last_kernel,
        in_specs=[WHOLE] * 6,
        out_specs=[ANYWHERE, WHOLE],
        out_shape=[
            jax.ShapeDtypeStruct((depth * peers, classes), f32),
            jax.ShapeDtypeStruct((2, rows), f32),
        ],
        scratch_shapes=[
            pltpu.VMEM((slots, depth * peers, widest), f32),
            pltpu.SemaphoreType.DMA((slots,)),
        ],
        compiler_params=grant(16),
    )(norm, trade(sent), places, flipped, near(residual), near(logits))
    return update, losses


def solution(mesh):
    placed = (P("row", None), P(AXES, None), P())
    return jax.shard_map(
        shards,
        mesh=mesh,
        in_specs=placed,
        out_specs=(P(None, AXES), P()),
        check_vma=False,
    )
```

```python
import functools

import jax
import jax.numpy as jnp
from jax import lax
from jax.experimental import pallas as pl
from jax.experimental.pallas import tpu as pltpu
from jax.sharding import PartitionSpec as P

AXES = ("cls", "row")
LANES = 128
LOG2E = 1.4426950408889634
MIB = 1 << 20

learn_rate = 2.0

WHOLE = pl.BlockSpec(memory_space=pltpu.VMEM)
ANYWHERE = pl.BlockSpec(memory_space=pltpu.HBM)


def blocks_of(width):
    step = next(t for t in (512, 256, 128) if width % t == 0)
    widths = [step] * (width // step)
    starts = [sum(widths[:k]) for k in range(len(widths))]
    return [slice(start, start + size) for start, size in zip(starts, widths)]


def diagonal():
    rows = lax.broadcasted_iota(jnp.int32, (LANES, LANES), 0)
    lanes = lax.broadcasted_iota(jnp.int32, (LANES, LANES), 1)
    return rows == lanes


def to_row(column):
    keep = diagonal()
    parts = []
    for start in range(0, column.shape[0], LANES):
        spread = jnp.broadcast_to(column[start : start + LANES], (LANES, LANES))
        parts.append(jnp.sum(jnp.where(keep, spread, 0.0), axis=0, keepdims=True))
    return jnp.concatenate(parts, axis=1)


def to_column(row):
    keep = diagonal()
    parts = []
    for start in range(0, row.shape[1], LANES):
        spread = jnp.broadcast_to(row[:, start : start + LANES], (LANES, LANES))
        parts.append(jnp.sum(jnp.where(keep, spread, 0.0), axis=1, keepdims=True))
    return jnp.concatenate(parts, axis=0)


def combine(masses):
    top = jnp.max(masses, axis=0)
    return top + jnp.log(jnp.sum(jnp.exp2(masses - top[None]), axis=0)) * LOG2E


def tally(logits, hits, first, peak_ref, mass_ref, pick_ref):
    groups = [logits[:, g : g + LANES] for g in range(0, logits.shape[1], LANES)]
    peak = functools.reduce(jnp.maximum, groups)
    if not first:
        peak = jnp.maximum(peak, peak_ref[...])
    mass = functools.reduce(jnp.add, [jnp.exp2(g - peak) for g in groups])
    pick = jnp.zeros_like(peak) if first else pick_ref[...]
    for g, h in zip(groups, hits):
        pick = jnp.where(h, g, pick)
    if not first:
        mass = mass + mass_ref[...] * jnp.exp2(peak_ref[...] - peak)
    peak_ref[...] = peak
    mass_ref[...] = mass
    pick_ref[...] = pick


def finish(peak_ref, mass_ref, pick_ref):
    lanes_peak = peak_ref[...]
    peak = jnp.max(lanes_peak, axis=1, keepdims=True)
    mass = jnp.sum(mass_ref[...] * jnp.exp2(lanes_peak - peak), axis=1, keepdims=True)
    pick = jnp.sum(pick_ref[...], axis=1, keepdims=True)
    return to_row(peak + jnp.log(mass) * LOG2E), to_row(pick)


def spread(row, peers):
    return jnp.broadcast_to(row[None], (peers, *row.shape))


def hits_of(places, columns_ref, block):
    rows = places.shape[0]
    places = places.reshape(rows // 8, 8, LANES)
    starts = range(block.start, block.stop, LANES)
    return [
        (places == columns_ref[:, g : g + LANES][None]).reshape(rows, LANES)
        for g in starts
    ]


def onehot(hits):
    return jnp.concatenate([jnp.where(h, 1.0, 0.0) for h in hits], axis=1)


def cast_kernel(in_hbm, out_hbm, wide_ref, slim_ref, in_sems, out_sems):
    ahead, chunk, _, width = slim_ref.shape
    steps = out_hbm.shape[0] // chunk

    def load(n):
        span = pl.ds(n * chunk * width, chunk * width)
        slot = n % ahead
        return pltpu.make_async_copy(in_hbm.at[:, span], wide_ref.at[slot], in_sems.at[slot])

    def store(n):
        slot = n % ahead
        return pltpu.make_async_copy(
            slim_ref.at[slot], out_hbm.at[pl.ds(n * chunk, chunk)], out_sems.at[slot]
        )

    for n in range(min(ahead, steps)):
        load(n).start()
    for n in range(steps):
        load(n).wait()
        if n >= ahead:
            store(n - ahead).wait()
        for k in range(chunk):
            piece = wide_ref[n % ahead, :, k * width : (k + 1) * width]
            slim_ref[n % ahead, k] = piece.astype(slim_ref.dtype)
        store(n).start()
        if n + ahead < steps:
            load(n + ahead).start()
    for n in range(max(0, steps - ahead), steps):
        store(n).wait()


def first_kernel(
    places_ref, columns_ref, x_hbm, w_hbm, logits_ref, sent_ref, x_ref, w_ref, peak_ref, mass_ref, pick_ref, sems
):
    stats = (peak_ref, mass_ref, pick_ref)
    depth = x_ref.shape[1]
    blocks = blocks_of(w_ref.shape[2])
    spans = [slice(0, blocks[0].stop), slice(blocks[0].stop, w_ref.shape[2])]
    copies = [pltpu.make_async_copy(x_hbm, x_ref, sems.at[2])]
    for n, span in enumerate(spans[: len(blocks)]):
        part = pl.ds(span.start, span.stop - span.start)
        copies.append(
            pltpu.make_async_copy(w_hbm.at[:, :, part], w_ref.at[:, :, part], sems.at[n])
        )
    for copy in copies:
        copy.start()
    places = places_ref[...]
    copies[0].wait()
    for k, block in enumerate(blocks):
        if k < 2:
            copies[k + 1].wait()
        taken = w_ref[:, :, block].reshape(depth, block.stop - block.start)
        logits = jnp.dot(x_ref[...], taken, preferred_element_type=jnp.float32) * LOG2E
        logits_ref[:, block] = logits
        if k % 2 or k == len(blocks) - 1:
            both = slice(blocks[k - k % 2].start, block.stop)
            tally(logits_ref[:, both], hits_of(places, columns_ref, both), k < 2, *stats)
    mass, pick = finish(*stats)
    peers, rows = sent_ref.shape[0], x_ref.shape[0]
    share = peers * LANES // rows
    sent_ref[:, :, :rows] = spread(mass, peers)
    for g in range(rows // LANES):
        sent_ref[g * share : (g + 1) * share, :, rows:] = spread(
            pick[:, g * LANES : (g + 1) * LANES], share
        )


def second_kernel(
    got_ref, places_ref, columns_ref, floats_ref, gram_ref, old_ref,
    residual_ref, logits_ref, norm_ref, sent_ref, peak_ref, mass_ref, pick_ref,
):
    rows = old_ref.shape[0]
    stats = (peak_ref, mass_ref, pick_ref)
    log_norm = combine(got_ref[:, :, :rows])
    norm_ref[...] = log_norm
    norm = to_column(log_norm)
    places = places_ref[...]
    labels = places.astype(jnp.float32)
    blocks = blocks_of(old_ref.shape[1])

    for k, block in enumerate(blocks):
        hits = hits_of(places, columns_ref, block)
        old = old_ref[:, block]
        residual = (jnp.exp2(old - norm) - onehot(hits)).astype(jnp.bfloat16)
        residual_ref[:, block] = residual
        logits = old - jnp.dot(
            gram_ref[...], residual_ref[:, block], preferred_element_type=jnp.float32
        )
        logits_ref[:, block] = logits
        if k % 2 or k == len(blocks) - 1:
            both = slice(blocks[k - k % 2].start, block.stop)
            tally(logits_ref[:, both], hits_of(labels, floats_ref, both), k < 2, *stats)
    mass, pick = finish(*stats)
    peers = sent_ref.shape[0]
    sent_ref[:, :, :rows] = spread(mass, peers)
    sent_ref[:, :, rows : 2 * rows] = spread(pick, peers)
    sent_ref[:, :, 2 * rows :] = spread(jnp.sum(got_ref[:, :, rows:], axis=0), peers)


def last_kernel(
    norm_ref, got_ref, places_ref, columns_ref, flipped_ref, residual_ref, logits_ref,
    update_hbm, losses_ref, update_ref, sems,
):
    rows = logits_ref.shape[0]
    share = got_ref.shape[0] * LANES // rows
    log_norm = combine(got_ref[:, :, :rows])
    pick = jnp.sum(got_ref[:, :, rows : 2 * rows], axis=0)
    old_pick = jnp.concatenate(
        [got_ref[g * share, :, 2 * rows :] for g in range(rows // LANES)], axis=1
    )
    losses = jnp.concatenate([norm_ref[...] - old_pick, log_norm - pick], axis=0)
    losses_ref[...] = losses * (1.0 / LOG2E)
    norm = to_column(log_norm)
    places = places_ref[...]
    blocks = blocks_of(logits_ref.shape[1])
    slots = update_ref.shape[0]

    def copy(k):
        size = blocks[k].stop - blocks[k].start
        return pltpu.make_async_copy(
            update_ref.at[k % slots, :, pl.ds(0, size)],
            update_hbm.at[:, pl.ds(blocks[k].start, size)],
            sems.at[k % slots],
        )

    for k, block in enumerate(blocks):
        chance = jnp.exp2(logits_ref[:, block] - norm)
        total = residual_ref[:, block].astype(jnp.float32)
        total = total + (chance - onehot(hits_of(places, columns_ref, block)))
        update = jnp.dot(
            flipped_ref[...], total.astype(jnp.bfloat16), preferred_element_type=jnp.float32
        )
        if k >= slots:
            copy(k - slots).wait()
        update_ref[k % slots, :, : block.stop - block.start] = update
        copy(k).start()
    for k in range(max(0, len(blocks) - slots), len(blocks)):
        copy(k).wait()


def grant(mib):
    return pltpu.CompilerParams(vmem_limit_bytes=mib * MIB)


def assemble_kernel(rate, sources_ref, *refs):
    *block_refs, x_ref, gram_ref, flipped_ref = refs
    height = block_refs[0].shape[0]
    for k, block_ref in enumerate(block_refs):
        x_ref[pl.ds(pl.multiple_of(sources_ref[k] * height, height), height), :] = block_ref[...]
    examples = x_ref[...]
    gram = lax.dot_general(
        examples, examples, (((1,), (1,)), ((), ())), preferred_element_type=jnp.float32
    )
    gram_ref[...] = (gram * (rate * LOG2E)).astype(gram_ref.dtype)
    flipped_ref[...] = (examples.T * -rate).astype(flipped_ref.dtype)


def neighbours(block):
    group = lax.axis_size("row")
    mine = lax.axis_index("row")
    paired = group & (group - 1) == 0
    sources, blocks = [mine], [block]
    for k in range(1, group):
        if paired:
            sources.append(mine ^ k)
            hops = [(i, i ^ k) for i in range(group)]
        else:
            sources.append((mine - k) % group)
            hops = [(i, (i + k) % group) for i in range(group)]
        blocks.append(lax.ppermute(block, "row", hops))
    return jnp.stack(sources).astype(jnp.int32), blocks


def near(array):
    return pltpu.with_memory_space_constraint(array, pltpu.VMEM)


def away(array):
    return pltpu.with_memory_space_constraint(array, pltpu.HBM)


def trade(sent):
    return lax.all_to_all(sent, AXES, 0, 0, tiled=True)


def shards(embeddings, weights, labels):
    peers = lax.axis_size(AXES)
    depth = weights.shape[0]
    classes = weights.shape[1] // peers
    f32, bf16 = jnp.float32, jnp.bfloat16
    chunk = 4 if peers % 4 == 0 else 1
    ahead = min(4, peers // chunk)
    pieces = pl.pallas_call(
        cast_kernel,
        in_specs=[ANYWHERE],
        out_specs=ANYWHERE,
        out_shape=pltpu.HBM((peers, depth, classes), bf16),
        scratch_shapes=[
            pltpu.VMEM((ahead, depth, chunk * classes), f32),
            pltpu.VMEM((ahead, chunk, depth, classes), bf16),
            pltpu.SemaphoreType.DMA((ahead,)),
            pltpu.SemaphoreType.DMA((ahead,)),
        ],
        compiler_params=grant(16),
    )(away(weights))
    block = lax.all_to_all(pieces, AXES, 0, 0, tiled=True)

    rows = labels.shape[0]
    rate = learn_rate / rows
    places = labels - lax.axis_index(AXES) * classes
    places = jnp.broadcast_to(places[:, None], (rows, LANES))
    sources, blocks = neighbours(embeddings.astype(bf16))
    examples, gram, flipped = pl.pallas_call(
        functools.partial(assemble_kernel, rate),
        in_specs=[pl.BlockSpec(memory_space=pltpu.SMEM)] + [WHOLE] * len(blocks),
        out_specs=[WHOLE] * 3,
        out_shape=[
            pltpu.HBM((rows, depth * peers), bf16),
            pltpu.HBM((rows, rows), bf16),
            pltpu.HBM((depth * peers, rows), bf16),
        ],
        compiler_params=grant(16),
    )(sources, *blocks)

    columns = lax.broadcasted_iota(jnp.int32, (8, classes), 1)
    places, columns, floats = lax.optimization_barrier((places, columns, columns.astype(f32)))
    logits_shape = pltpu.VMEM((rows, classes), f32)
    scratch = [pltpu.VMEM((rows, LANES), f32)] * 3
    blocks = blocks_of(classes)
    widest, slots = max(b.stop - b.start for b in blocks), min(3, len(blocks))
    logits, sent = pl.pallas_call(
        first_kernel,
        in_specs=[WHOLE, WHOLE, ANYWHERE, ANYWHERE],
        out_specs=[WHOLE] * 2,
        out_shape=[logits_shape, jax.ShapeDtypeStruct((peers, 1, rows + LANES), f32)],
        scratch_shapes=[
            pltpu.VMEM(examples.shape, bf16),
            pltpu.VMEM(block.shape, bf16),
            *scratch,
            pltpu.SemaphoreType.DMA((3,)),
        ],
        compiler_params=grant(16),
    )(places, columns, away(examples), away(block))
    residual, logits, norm, sent = pl.pallas_call(
        second_kernel,
        in_specs=[WHOLE] * 6,
        out_specs=[WHOLE] * 4,
        out_shape=[
            pltpu.VMEM((rows, classes), bf16),
            logits_shape,
            jax.ShapeDtypeStruct((1, rows), f32),
            jax.ShapeDtypeStruct((peers, 1, 2 * rows + LANES), f32),
        ],
        scratch_shapes=scratch,
        compiler_params=grant(17),
    )(trade(sent), places, columns, floats, gram, near(logits))
    update, losses = pl.pallas_call(
        last_kernel,
        in_specs=[WHOLE] * 7,
        out_specs=[ANYWHERE, WHOLE],
        out_shape=[
            jax.ShapeDtypeStruct((depth * peers, classes), f32),
            jax.ShapeDtypeStruct((2, rows), f32),
        ],
        scratch_shapes=[
            pltpu.VMEM((slots, depth * peers, widest), f32),
            pltpu.SemaphoreType.DMA((slots,)),
        ],
        compiler_params=grant(16),
    )(norm, trade(sent), places, columns, flipped, near(residual), near(logits))
    return update, losses


def solution(mesh):
    placed = (P("row", None), P(AXES, None), P())
    return jax.shard_map(
        shards,
        mesh=mesh,
        in_specs=placed,
        out_specs=(P(None, AXES), P()),
        check_vma=False,
    )
```

```python
import functools

import jax
import jax.numpy as jnp
from jax import lax
from jax.experimental import pallas as pl
from jax.experimental.pallas import tpu as pltpu
from jax.sharding import PartitionSpec as P

AXES = ("cls", "row")
LANES = 128
LOG2E = 1.4426950408889634
MIB = 1 << 20

learn_rate = 2.0

WHOLE = pl.BlockSpec(memory_space=pltpu.VMEM)
ANYWHERE = pl.BlockSpec(memory_space=pltpu.HBM)


def blocks_of(width):
    step = next(t for t in (512, 256, 128) if width % t == 0)
    widths = [step] * (width // step)
    starts = [sum(widths[:k]) for k in range(len(widths))]
    return [slice(start, start + size) for start, size in zip(starts, widths)]


def wide_blocks(width):
    blocks = blocks_of(width)
    pairs = [blocks[k : k + 2] for k in range(0, len(blocks), 2)]
    return [slice(pair[0].start, pair[-1].stop) for pair in pairs]


def diagonal():
    rows = lax.broadcasted_iota(jnp.int32, (LANES, LANES), 0)
    lanes = lax.broadcasted_iota(jnp.int32, (LANES, LANES), 1)
    return rows == lanes


def to_row(column):
    keep = diagonal()
    parts = []
    for start in range(0, column.shape[0], LANES):
        spread = jnp.broadcast_to(column[start : start + LANES], (LANES, LANES))
        parts.append(jnp.sum(jnp.where(keep, spread, 0.0), axis=0, keepdims=True))
    return jnp.concatenate(parts, axis=1)


def to_column(row):
    keep = diagonal()
    parts = []
    for start in range(0, row.shape[1], LANES):
        spread = jnp.broadcast_to(row[:, start : start + LANES], (LANES, LANES))
        parts.append(jnp.sum(jnp.where(keep, spread, 0.0), axis=1, keepdims=True))
    return jnp.concatenate(parts, axis=0)


def combine(masses):
    top = jnp.max(masses, axis=0)
    return top + jnp.log(jnp.sum(jnp.exp2(masses - top[None]), axis=0)) * LOG2E


def tally(logits, hits, first, peak_ref, mass_ref, pick_ref):
    groups = [logits[:, g : g + LANES] for g in range(0, logits.shape[1], LANES)]
    peak = functools.reduce(jnp.maximum, groups)
    if not first:
        peak = jnp.maximum(peak, peak_ref[...])
    mass = functools.reduce(jnp.add, [jnp.exp2(g - peak) for g in groups])
    pick = jnp.zeros_like(peak) if first else pick_ref[...]
    for g, h in zip(groups, hits):
        pick = jnp.where(h, g, pick)
    if not first:
        mass = mass + mass_ref[...] * jnp.exp2(peak_ref[...] - peak)
    peak_ref[...] = peak
    mass_ref[...] = mass
    pick_ref[...] = pick


def finish(peak_ref, mass_ref, pick_ref):
    lanes_peak = peak_ref[...]
    peak = jnp.max(lanes_peak, axis=1, keepdims=True)
    mass = jnp.sum(mass_ref[...] * jnp.exp2(lanes_peak - peak), axis=1, keepdims=True)
    pick = jnp.sum(pick_ref[...], axis=1, keepdims=True)
    return to_row(peak + jnp.log(mass) * LOG2E), to_row(pick)


def spread(row, peers):
    return jnp.broadcast_to(row[None], (peers, *row.shape))


def hits_of(places, columns_ref, block):
    rows = places.shape[0]
    places = places.reshape(rows // 8, 8, LANES)
    starts = range(block.start, block.stop, LANES)
    return [
        (places == columns_ref[:, g : g + LANES][None]).reshape(rows, LANES)
        for g in starts
    ]


def onehot(hits):
    return jnp.concatenate([jnp.where(h, 1.0, 0.0) for h in hits], axis=1)


def cast_kernel(in_hbm, out_hbm, wide_ref, slim_ref, in_sems, out_sems):
    ahead, chunk, _, width = slim_ref.shape
    steps = out_hbm.shape[0] // chunk

    def load(n):
        span = pl.ds(n * chunk * width, chunk * width)
        slot = n % ahead
        return pltpu.make_async_copy(in_hbm.at[:, span], wide_ref.at[slot], in_sems.at[slot])

    def store(n):
        slot = n % ahead
        return pltpu.make_async_copy(
            slim_ref.at[slot], out_hbm.at[pl.ds(n * chunk, chunk)], out_sems.at[slot]
        )

    for n in range(min(ahead, steps)):
        load(n).start()
    for n in range(steps):
        load(n).wait()
        if n >= ahead:
            store(n - ahead).wait()
        for k in range(chunk):
            piece = wide_ref[n % ahead, :, k * width : (k + 1) * width]
            slim_ref[n % ahead, k] = piece.astype(slim_ref.dtype)
        store(n).start()
        if n + ahead < steps:
            load(n + ahead).start()
    for n in range(max(0, steps - ahead), steps):
        store(n).wait()


def first_kernel(
    places_ref, columns_ref, x_hbm, w_hbm, logits_ref, sent_ref, x_ref, w_ref, peak_ref, mass_ref, pick_ref, sems
):
    stats = (peak_ref, mass_ref, pick_ref)
    depth = x_ref.shape[1]
    blocks = blocks_of(w_ref.shape[2])
    spans = [slice(0, blocks[0].stop), slice(blocks[0].stop, w_ref.shape[2])]
    copies = [pltpu.make_async_copy(x_hbm, x_ref, sems.at[2])]
    for n, span in enumerate(spans[: len(blocks)]):
        part = pl.ds(span.start, span.stop - span.start)
        copies.append(
            pltpu.make_async_copy(w_hbm.at[:, :, part], w_ref.at[:, :, part], sems.at[n])
        )
    for copy in copies:
        copy.start()
    places = places_ref[...]
    copies[0].wait()
    for k, block in enumerate(blocks):
        if k < 2:
            copies[k + 1].wait()
        taken = w_ref[:, :, block].reshape(depth, block.stop - block.start)
        logits = jnp.dot(x_ref[...], taken, preferred_element_type=jnp.float32) * LOG2E
        logits_ref[:, block] = logits
        if k % 2 or k == len(blocks) - 1:
            both = slice(blocks[k - k % 2].start, block.stop)
            tally(logits_ref[:, both], hits_of(places, columns_ref, both), k < 2, *stats)
    mass, pick = finish(*stats)
    peers, rows = sent_ref.shape[0], x_ref.shape[0]
    share = peers * LANES // rows
    sent_ref[:, :, :rows] = spread(mass, peers)
    for g in range(rows // LANES):
        sent_ref[g * share : (g + 1) * share, :, rows:] = spread(
            pick[:, g * LANES : (g + 1) * LANES], share
        )


def second_kernel(
    got_ref, places_ref, columns_ref, floats_ref, gram_ref, old_ref,
    residual_ref, logits_ref, norm_ref, sent_ref, peak_ref, mass_ref, pick_ref,
):
    rows = old_ref.shape[0]
    stats = (peak_ref, mass_ref, pick_ref)
    log_norm = combine(got_ref[:, :, :rows])
    norm_ref[...] = log_norm
    norm = to_column(log_norm)
    places = places_ref[...]
    labels = places.astype(jnp.float32)
    blocks = blocks_of(old_ref.shape[1])

    for k, block in enumerate(blocks):
        hits = hits_of(places, columns_ref, block)
        old = old_ref[:, block]
        residual = (jnp.exp2(old - norm) - onehot(hits)).astype(jnp.bfloat16)
        residual_ref[:, block] = residual
        logits = old - jnp.dot(
            gram_ref[...], residual_ref[:, block], preferred_element_type=jnp.float32
        )
        logits_ref[:, block] = logits
        if k % 2 or k == len(blocks) - 1:
            both = slice(blocks[k - k % 2].start, block.stop)
            tally(logits_ref[:, both], hits_of(labels, floats_ref, both), k < 2, *stats)
    mass, pick = finish(*stats)
    peers = sent_ref.shape[0]
    sent_ref[:, :, :rows] = spread(mass, peers)
    sent_ref[:, :, rows : 2 * rows] = spread(pick, peers)
    sent_ref[:, :, 2 * rows :] = spread(jnp.sum(got_ref[:, :, rows:], axis=0), peers)


def last_kernel(
    norm_ref, got_ref, places_ref, columns_ref, flipped_ref, residual_ref, logits_ref,
    update_hbm, losses_ref, update_ref, sems,
):
    rows = logits_ref.shape[0]
    share = got_ref.shape[0] * LANES // rows
    log_norm = combine(got_ref[:, :, :rows])
    pick = jnp.sum(got_ref[:, :, rows : 2 * rows], axis=0)
    old_pick = jnp.concatenate(
        [got_ref[g * share, :, 2 * rows :] for g in range(rows // LANES)], axis=1
    )
    losses = jnp.concatenate([norm_ref[...] - old_pick, log_norm - pick], axis=0)
    losses_ref[...] = losses * (1.0 / LOG2E)
    norm = to_column(log_norm)
    places = places_ref[...]
    blocks = wide_blocks(logits_ref.shape[1])
    slots = update_ref.shape[0]

    def copy(k):
        size = blocks[k].stop - blocks[k].start
        return pltpu.make_async_copy(
            update_ref.at[k % slots, :, pl.ds(0, size)],
            update_hbm.at[:, pl.ds(blocks[k].start, size)],
            sems.at[k % slots],
        )

    for k, block in enumerate(blocks):
        chance = jnp.exp2(logits_ref[:, block] - norm)
        total = residual_ref[:, block].astype(jnp.float32)
        total = total + (chance - onehot(hits_of(places, columns_ref, block)))
        update = jnp.dot(
            flipped_ref[...], total.astype(jnp.bfloat16), preferred_element_type=jnp.float32
        )
        if k >= slots:
            copy(k - slots).wait()
        update_ref[k % slots, :, : block.stop - block.start] = update
        copy(k).start()
    for k in range(max(0, len(blocks) - slots), len(blocks)):
        copy(k).wait()


def grant(mib):
    return pltpu.CompilerParams(vmem_limit_bytes=mib * MIB)


def assemble_kernel(rate, sources_ref, *refs):
    *block_refs, x_ref, gram_ref, flipped_ref = refs
    height = block_refs[0].shape[0]
    for k, block_ref in enumerate(block_refs):
        x_ref[pl.ds(pl.multiple_of(sources_ref[k] * height, height), height), :] = block_ref[...]
    examples = x_ref[...]
    gram = lax.dot_general(
        examples, examples, (((1,), (1,)), ((), ())), preferred_element_type=jnp.float32
    )
    gram_ref[...] = (gram * (rate * LOG2E)).astype(gram_ref.dtype)
    flipped_ref[...] = (examples.T * -rate).astype(flipped_ref.dtype)


def neighbours(block):
    group = lax.axis_size("row")
    mine = lax.axis_index("row")
    paired = group & (group - 1) == 0
    sources, blocks = [mine], [block]
    for k in range(1, group):
        if paired:
            sources.append(mine ^ k)
            hops = [(i, i ^ k) for i in range(group)]
        else:
            sources.append((mine - k) % group)
            hops = [(i, (i + k) % group) for i in range(group)]
        blocks.append(lax.ppermute(block, "row", hops))
    return jnp.stack(sources).astype(jnp.int32), blocks


def near(array):
    return pltpu.with_memory_space_constraint(array, pltpu.VMEM)


def away(array):
    return pltpu.with_memory_space_constraint(array, pltpu.HBM)


def trade(sent):
    return lax.all_to_all(sent, AXES, 0, 0, tiled=True)


def shards(embeddings, weights, labels):
    peers = lax.axis_size(AXES)
    depth = weights.shape[0]
    classes = weights.shape[1] // peers
    f32, bf16 = jnp.float32, jnp.bfloat16
    chunk = 4 if peers % 4 == 0 else 1
    ahead = min(4, peers // chunk)
    pieces = pl.pallas_call(
        cast_kernel,
        in_specs=[ANYWHERE],
        out_specs=ANYWHERE,
        out_shape=pltpu.HBM((peers, depth, classes), bf16),
        scratch_shapes=[
            pltpu.VMEM((ahead, depth, chunk * classes), f32),
            pltpu.VMEM((ahead, chunk, depth, classes), bf16),
            pltpu.SemaphoreType.DMA((ahead,)),
            pltpu.SemaphoreType.DMA((ahead,)),
        ],
        compiler_params=grant(16),
    )(away(weights))
    block = lax.all_to_all(pieces, AXES, 0, 0, tiled=True)

    rows = labels.shape[0]
    rate = learn_rate / rows
    places = labels - lax.axis_index(AXES) * classes
    places = jnp.broadcast_to(places[:, None], (rows, LANES))
    sources, blocks = neighbours(embeddings.astype(bf16))
    examples, gram, flipped = pl.pallas_call(
        functools.partial(assemble_kernel, rate),
        in_specs=[pl.BlockSpec(memory_space=pltpu.SMEM)] + [WHOLE] * len(blocks),
        out_specs=[WHOLE] * 3,
        out_shape=[
            pltpu.HBM((rows, depth * peers), bf16),
            pltpu.HBM((rows, rows), bf16),
            pltpu.HBM((depth * peers, rows), bf16),
        ],
        compiler_params=grant(16),
    )(sources, *blocks)

    columns = lax.broadcasted_iota(jnp.int32, (8, classes), 1)
    places, columns, floats = lax.optimization_barrier((places, columns, columns.astype(f32)))
    logits_shape = pltpu.VMEM((rows, classes), f32)
    scratch = [pltpu.VMEM((rows, LANES), f32)] * 3
    blocks = blocks_of(classes)
    wide = wide_blocks(classes)
    widest, slots = max(b.stop - b.start for b in wide), min(2, len(wide))
    logits, sent = pl.pallas_call(
        first_kernel,
        in_specs=[WHOLE, WHOLE, ANYWHERE, ANYWHERE],
        out_specs=[WHOLE] * 2,
        out_shape=[logits_shape, jax.ShapeDtypeStruct((peers, 1, rows + LANES), f32)],
        scratch_shapes=[
            pltpu.VMEM(examples.shape, bf16),
            pltpu.VMEM(block.shape, bf16),
            *scratch,
            pltpu.SemaphoreType.DMA((3,)),
        ],
        compiler_params=grant(16),
    )(places, columns, away(examples), away(block))
    residual, logits, norm, sent = pl.pallas_call(
        second_kernel,
        in_specs=[WHOLE] * 6,
        out_specs=[WHOLE] * 4,
        out_shape=[
            pltpu.VMEM((rows, classes), bf16),
            logits_shape,
            jax.ShapeDtypeStruct((1, rows), f32),
            jax.ShapeDtypeStruct((peers, 1, 2 * rows + LANES), f32),
        ],
        scratch_shapes=scratch,
        compiler_params=grant(17),
    )(trade(sent), places, columns, floats, gram, near(logits))
    update, losses = pl.pallas_call(
        last_kernel,
        in_specs=[WHOLE] * 7,
        out_specs=[ANYWHERE, WHOLE],
        out_shape=[
            jax.ShapeDtypeStruct((depth * peers, classes), f32),
            jax.ShapeDtypeStruct((2, rows), f32),
        ],
        scratch_shapes=[
            pltpu.VMEM((slots, depth * peers, widest), f32),
            pltpu.SemaphoreType.DMA((slots,)),
        ],
        compiler_params=grant(18),
    )(norm, trade(sent), places, columns, flipped, near(residual), near(logits))
    return update, losses


def solution(mesh):
    placed = (P("row", None), P(AXES, None), P())
    return jax.shard_map(
        shards,
        mesh=mesh,
        in_specs=placed,
        out_specs=(P(None, AXES), P()),
        check_vma=False,
    )
```
